32 devices in a mesh: field: 8 (over y, x, core), slab: 4 (over z).
Axes of the slice: x: 2, y: 2, z: 4, core: 2. Of those that a mesh axis runs over, the one named last changes fastest.
Arguments:
- fields: float32 [32, 16, 16, 16, 128], P('field', None, 'slab'), may hold values from -6 to 6
- velocity: float32 [3, 16, 16, 128], P(None, 'slab'), may hold values from -0.15 to 0.15
- diffusivity: float32 [16, 16, 128], P('slab'), may hold values from 0.06 to 0.14
- noise: float32 [32, 4, 3], P('field'), may hold values from -0.8 to 0.8
- mix_rate: float32 [16, 16, 128], P('slab'), may hold values from 0.2 to 1
- evaporation: float32 [16, 16, 128], P('slab'), may hold values from 0.05 to 0.5
- rate_matrix: float32 [32, 16], replicated, may hold values from -1.5 to 1.5
- stoich: float32 [16, 32], replicated, may hold values from -1 to 1
- prefactor: float32 [32], replicated, may hold values from 0.05 to 0.5
Outputs:
- updated: float32 [32, 16, 16, 16, 128], P('field', None, 'slab')
The draws below stay inside these ranges and needn't reach their ends.
All inputs are finite; a program needn't handle non-finite values.
Results may differ from the reference program's by a relative error of at most 0.000073.
Values sent between devices are 32-bit elements; how exact they have to be, the bound alone decides.
A program may use at most 64 MiB of HBM per device.

```python
import math
import jax
import jax.numpy as jnp
from jax import lax

F = 32
S = 16
R = 32
SUBSTEPS = 4
NZ = 16
NY = 128
NX = 16


def levels(stream_key, extent, shards, least, top_value):
    factor_of = 1.0
    for position, shards_of in shards:
        heights = jax.random.uniform(jax.random.fold_in(jax.random.fold_in(stream_key, 6), position), (shards_of,), jnp.float32, least / len(shards), top_value / len(shards))
        factor_of = factor_of * jnp.repeat(jnp.exp(heights), extent[position] // shards_of).reshape((-1,) + (1,) * (len(extent) - 1 - position))
    return factor_of


def centred(stream_key, extent, scale, reach, split=(), kind=jnp.bfloat16):
    entries = scale * jax.random.normal(stream_key, extent, jnp.float32)
    if split:
        entries = entries * levels(stream_key, extent, split, -0.22, 0.18)
    return jnp.clip(entries, -reach, reach).astype(kind)


def setup_inputs(seed: int = 0) -> dict:
    key_of = jax.random.split(jax.random.key(seed), 10)
    fields = centred(key_of[0], (F, S, NX, NZ, NY), 1.0, 6.0, ((0, 8), (2, 4)), jnp.float32)
    velocity = jnp.clip(jax.random.uniform(key_of[1], (3, NX, NZ, NY), jnp.float32, -0.15, 0.15) * levels(key_of[1], (3, NX, NZ, NY), ((1, 4),), -0.4, 0.0), -0.15, 0.15)
    diffusivity = jnp.clip(0.06 + 0.08 * jax.random.uniform(key_of[2], (NX, NZ, NY), jnp.float32) ** levels(key_of[2], (NX, NZ, NY), ((0, 4),), -0.2, 0.2), 0.06, 0.14)
    noise = centred(key_of[3], (F, SUBSTEPS, 3), 0.2, 0.8, ((0, 8),), jnp.float32)
    mix_rate = jnp.clip(jnp.exp(math.log(1.0) - 1.609438 * jax.random.uniform(key_of[4], (NX, NZ, NY), jnp.float32) ** levels(key_of[4], (NX, NZ, NY), ((0, 4),), -0.2, 0.2)), 0.2, 1.0)
    evaporation = jnp.clip(jnp.exp(math.log(0.5) - 2.3025851 * jax.random.uniform(key_of[5], (NX, NZ, NY), jnp.float32) ** levels(key_of[5], (NX, NZ, NY), ((0, 4),), -0.2, 0.2)), 0.05, 0.5)
    rate_matrix = centred(key_of[6], (R, S), S ** -0.5, 1.5, (), jnp.float32)
    stoich = centred(key_of[7], (S, R), R ** -0.5, 1.0, (), jnp.float32)
    prefactor = jnp.clip(jnp.exp(jax.random.uniform(key_of[8], (R,), jnp.float32, math.log(0.05), math.log(0.5))), 0.05, 0.5)
    return dict(fields=fields, velocity=velocity, diffusivity=diffusivity, noise=noise, mix_rate=mix_rate, evaporation=evaporation, rate_matrix=rate_matrix, stoich=stoich, prefactor=prefactor)


def advance(padded, velocity, diffusivity, drifts):
    center = padded[:, :, 1:-1]
    x_ahead = padded[:, :, 2:]
    x_behind = padded[:, :, :-2]
    y_ahead = jnp.roll(center, -1, axis=4)
    y_behind = jnp.roll(center, 1, axis=4)
    z_ahead = jnp.roll(center, -1, axis=3)
    z_behind = jnp.roll(center, 1, axis=3)
    spread = x_ahead + x_behind + y_ahead + y_behind + z_ahead + z_behind - 6.0 * center
    stir_scale = jnp.sqrt(2.0 * diffusivity)
    drift_x = velocity[0] - stir_scale * drifts[:, 0][:, None, None, None, None]
    drift_y = velocity[1] - stir_scale * drifts[:, 1][:, None, None, None, None]
    drift_z = velocity[2] - stir_scale * drifts[:, 2][:, None, None, None, None]
    carried = drift_x * (x_ahead - x_behind) * 0.5 + drift_y * (y_ahead - y_behind) * 0.5 + drift_z * (z_ahead - z_behind) * 0.5
    return center + diffusivity * spread - carried

def react(states, average, rates, vapour, rate_matrix, stoich, prefactor):
    species = states.shape[1]
    fuel = (jnp.arange(species) == 0).astype(jnp.float32)
    mixed = states - 0.5 * rates * (states - average) + vapour * fuel[:, None]
    drive = jnp.einsum('rs,ksc->krc', rate_matrix, mixed, precision=lax.Precision.HIGHEST)
    speed = prefactor[None, :, None] * jnp.exp(2.0 * jnp.tanh(drive))
    return mixed + jnp.einsum('sr,krc->ksc', stoich, speed, precision=lax.Precision.HIGHEST)

def reference(fields, velocity, diffusivity, noise, mix_rate, evaporation, rate_matrix, stoich, prefactor):

    def carry_field(packed):
        state, drifts = packed
        state = state[None]
        for substep in range(SUBSTEPS):
            padded = jnp.pad(state, ((0, 0), (0, 0), (1, 1), (0, 0), (0, 0)))
            state = advance(padded, velocity, diffusivity, drifts[substep][None])
        return state[0]
    moved = lax.map(carry_field, (fields, noise))
    average = (lax.optimization_barrier(jnp.sum(moved, axis=0)) / F).reshape(S, -1)
    rates = mix_rate.reshape(-1)
    vapour = evaporation.reshape(-1)

    def react_field(state):
        result = react(state.reshape(1, S, -1), average, rates, vapour, rate_matrix, stoich, prefactor)
        return result[0].reshape(state.shape)
    return lax.map(react_field, moved)
```

```python
import functools

import jax
import jax.numpy as jnp
from jax import lax
from jax.experimental import pallas as pl
from jax.experimental.pallas import tpu as pltpu
from jax.sharding import PartitionSpec as P

GROUP = 2
LANES = 4
DELAYS = (2, 2, 2, 2, 2, 2, 2)
ROWS = 8


def schedule(groups, substeps, stages):
    width = min(LANES, groups)
    events = []
    slot = 0
    for first in range(0, groups, width):
        wave = range(first, min(first + width, groups))
        for k in range(substeps):
            for g in wave:
                events.append((slot, 1, "move", g, k))
                if k == substeps - 1:
                    when = slot
                    for stage in range(stages):
                        when += DELAYS[stage % len(DELAYS)]
                        events.append((when, 0, "sum", g, stage))
                slot += 1
    return width, [e[2:] for e in sorted(events, key=lambda e: (e[0], e[1]))]


def expand(small, row_of, col_of):
    rows, cols = small.shape
    tall = lax.broadcasted_iota(jnp.int32, (rows * ROWS, rows), 0) // ROWS
    pick_row = (tall == lax.broadcasted_iota(jnp.int32, (rows * ROWS, rows), 1)).astype(jnp.bfloat16)
    wide = lax.broadcasted_iota(jnp.int32, (cols, cols * ROWS), 1) // ROWS
    pick_col = (wide == lax.broadcasted_iota(jnp.int32, (cols, cols * ROWS), 0)).astype(jnp.bfloat16)
    half = jnp.dot(pick_row, small, preferred_element_type=jnp.float32).astype(jnp.bfloat16)
    full = jnp.dot(half, pick_col, preferred_element_type=jnp.float32)
    shape = (rows * ROWS, cols * ROWS)
    same = (lax.broadcasted_iota(jnp.int32, shape, 0) % ROWS) == (
        lax.broadcasted_iota(jnp.int32, shape, 1) % ROWS
    )
    return jnp.where(same, full, 0.0).astype(jnp.bfloat16)


def halves(value):
    high = value.astype(jnp.bfloat16)
    low = (value - high.astype(jnp.float32)).astype(jnp.bfloat16)
    return high, low


def kernel(
    slabs, peers, substeps,
    x_hbm, vel, diff, noise, rate, vapour, matrix, stoich, pref,
    out_hbm,
    st, halo, planes, part, got, acc, tot, xs, outv, a_one, a_two, b_all,
    in_sem, out_sem, hs_sem, hr_sem, rs_sem, rr_sem,
):
    fields, species, nx, nz, ny = x_hbm.shape
    reactions = matrix.shape[0]
    groups = species // GROUP
    bits = peers.bit_length() - 1
    stages = bits + 1
    half = nx // 2
    total_fields = fields * peers
    blocks = nz // ROWS

    def members(g):
        return pl.ds(g * GROUP, GROUP)

    loads = [
        pltpu.make_async_copy(x_hbm.at[:, members(g)], st.at[0, :, members(g)], in_sem.at[g])
        for g in range(groups)
    ]
    for load in loads:
        load.start()

    me = lax.axis_index("slab")
    seat = lax.axis_index("field")

    def partner(bit):
        step = 1 << bit
        return seat + step * (1 - 2 * ((seat // step) % 2))

    core = seat % 2
    mine = pl.ds(core * half, half)
    theirs = pl.ds((1 - core) * half, half)

    barrier = pltpu.get_barrier_semaphore()

    @pl.when(me > 0)
    def _():
        pl.semaphore_signal(barrier, inc=1, device_id={"slab": me - 1})

    @pl.when(me < slabs - 1)
    def _():
        pl.semaphore_signal(barrier, inc=1, device_id={"slab": me + 1})

    for bit in range(bits):
        pl.semaphore_signal(barrier, inc=1, device_id={"field": partner(bit)})
    has_left = (me + slabs - 1) // slabs
    has_right = 1 - (me + 1) // slabs
    pl.semaphore_wait(barrier, bits + has_left + has_right)

    def to_left(g, k):
        source = x_hbm.at[:, members(g), 0] if k == 0 else st.at[k, :, members(g), 0]
        return pltpu.make_async_remote_copy(
            src_ref=source, dst_ref=halo.at[k, 1, :, members(g)],
            send_sem=hs_sem.at[k, 0, g], recv_sem=hr_sem.at[k, 1, g],
            device_id={"slab": me - 1},
        )

    def to_right(g, k):
        source = x_hbm.at[:, members(g), nx - 1] if k == 0 else st.at[k, :, members(g), nx - 1]
        return pltpu.make_async_remote_copy(
            src_ref=source, dst_ref=halo.at[k, 0, :, members(g)],
            send_sem=hs_sem.at[k, 1, g], recv_sem=hr_sem.at[k, 0, g],
            device_id={"slab": me + 1},
        )

    def send_halo(g, k):
        @pl.when(me > 0)
        def _():
            to_left(g, k).start()

        @pl.when(me < slabs - 1)
        def _():
            to_right(g, k).start()

    def wait_halo(g, k):
        @pl.when(me > 0)
        def _():
            to_right(g, k).wait_recv()

        @pl.when(me < slabs - 1)
        def _():
            to_left(g, k).wait_recv()

    width, events = schedule(groups, substeps, stages)
    for g in range(width):
        send_halo(g, 0)

    @pl.when(me == 0)
    def _():
        for k in range(substeps):
            @pl.loop(0, fields)
            def _(f):
                halo[k, 0, f] = jnp.zeros((species, nz, ny), jnp.float32)

    @pl.when(me == slabs - 1)
    def _():
        for k in range(substeps):
            @pl.loop(0, fields)
            def _(f):
                halo[k, 1, f] = jnp.zeros((species, nz, ny), jnp.float32)

    for x in range(nx):
        d = diff[x]
        for i in range(3):
            planes[x, i] = d - 0.5 * vel[i, x]
        planes[x, 3] = 0.5 * jnp.sqrt(2.0 * d)
        planes[x, 4] = 2.0 * d
        planes[x, 5] = 1.0 - 6.0 * d

    w_high, w_low = halves(matrix[...])
    a_high = expand(w_high, ROWS, ROWS)
    a_one[...] = jnp.concatenate([a_high, a_high], axis=1)
    a_two[...] = expand(w_low, ROWS, ROWS)
    s_high, s_low = halves(stoich[...] * pref[...])
    b_high = expand(s_high, ROWS, ROWS)
    b_all[...] = jnp.concatenate([b_high, b_high, expand(s_low, ROWS, ROWS)], axis=1)

    def exchange(g, stage):
        if stage == 0:
            source, target, bit = part.at[members(g), theirs], got.at[0, members(g)], 0
        elif stage < bits:
            source, target, bit = acc.at[stage - 1, members(g)], got.at[stage, members(g)], stage
        else:
            source, target, bit = tot.at[members(g), mine], tot.at[members(g), mine], 0
        return pltpu.make_async_remote_copy(
            src_ref=source, dst_ref=target,
            send_sem=rs_sem.at[stage, g], recv_sem=rr_sem.at[stage, g],
            device_id={"field": partner(bit)},
        )

    def move(g, k):
        if k == 0:
            loads[g].wait()
        wait_halo(g, k)

        @pl.loop(0, fields)
        def _(f):
            shift = [noise[f, k, i] for i in range(3)]
            for x in range(nx):
                root = planes[x, 3]
                twice = planes[x, 4]
                diag = planes[x, 5]
                ahead = [planes[x, i] + root * shift[i] for i in range(3)]
                behind = [twice - a for a in ahead]
                for s in range(g * GROUP, (g + 1) * GROUP):
                    c = st[k, f, s, x]
                    xa = st[k, f, s, x + 1] if x + 1 < nx else halo[k, 1, f, s]
                    xb = st[k, f, s, x - 1] if x > 0 else halo[k, 0, f, s]
                    ya = pltpu.roll(c, ny - 1, 1)
                    yb = pltpu.roll(c, 1, 1)
                    za = pltpu.roll(c, nz - 1, 0)
                    zb = pltpu.roll(c, 1, 0)
                    st[k + 1, f, s, x] = (
                        (diag * c + (ahead[0] * xa + behind[0] * xb))
                        + (ahead[1] * ya + behind[1] * yb)
                        + (ahead[2] * za + behind[2] * zb)
                    )

        if k < substeps - 1:
            send_halo(g, k + 1)
            if k == substeps - 2 and g + width < groups:
                send_halo(g + width, 0)
        else:
            for s in range(g * GROUP, (g + 1) * GROUP):
                for x in range(nx):
                    part[s, x] = functools.reduce(
                        lambda a, b: a + b, [st[substeps, f, s, x] for f in range(fields)]
                    )
            exchange(g, 0).start()

    def mix(g):
        @pl.loop(0, fields)
        def _(f):
            for x in range(nx):
                half_rate = 0.5 * rate[x]
                for s in range(g * GROUP, (g + 1) * GROUP, 2):
                    pair = []
                    for one in (s, s + 1):
                        m = st[substeps, f, one, x]
                        m = m - half_rate * (m - tot[one, x] * (1.0 / total_fields))
                        if one == 0:
                            m = m + vapour[x]
                        outv[f, one, x] = m
                        pair.append(m)
                    for b in range(blocks):
                        rows = jnp.concatenate([m[b * ROWS:(b + 1) * ROWS] for m in pair], axis=0)
                        high, low = halves(rows)
                        lanes = slice(b * ny, (b + 1) * ny)
                        xs[f * nx + x, s * ROWS:(s + 2) * ROWS, lanes] = high
                        xs[f * nx + x, (species + s) * ROWS:(species + s + 2) * ROWS, lanes] = low

    def reduce_step(g, stage):
        exchange(g, stage).wait_recv()
        if stage == bits:
            mix(g)
            return
        for s in range(g * GROUP, (g + 1) * GROUP):
            held = part[s, mine] if stage == 0 else acc[stage - 1, s]
            value = held + got[stage, s]
            if stage == bits - 1:
                tot[s, mine] = value
            else:
                acc[stage, s] = value
        exchange(g, stage + 1).start()

    for kind, g, k in events:
        if kind == "move":
            move(g, k)
        else:
            reduce_step(g, k)

    def store(i):
        f, x = i // nx, i % nx
        return pltpu.make_async_copy(outv.at[f, :, x], out_hbm.at[f, :, x], out_sem.at[i])

    @pl.loop(0, fields * nx)
    def _(i):
        f, x = i // nx, i % nx
        drive = jnp.dot(a_one[...], xs[i], preferred_element_type=jnp.float32)
        drive = drive + jnp.dot(
            a_two[...], xs[i, : species * ROWS], preferred_element_type=jnp.float32
        )
        speed = jnp.exp(2.0 * jnp.tanh(drive))
        high, low = halves(speed)
        gain = jnp.dot(
            b_all[...], jnp.concatenate([high, low, high], axis=0),
            preferred_element_type=jnp.float32,
        )
        for b in range(blocks):
            piece = gain[:, b * ny:(b + 1) * ny].reshape(species, ROWS, ny)
            outv[f, :, x, b * ROWS:(b + 1) * ROWS] += piece
        store(i).start()

    for k in range(substeps):
        for g in range(groups):
            @pl.when(me > 0)
            def _():
                to_left(g, k).wait_send()

            @pl.when(me < slabs - 1)
            def _():
                to_right(g, k).wait_send()

    for g in range(groups):
        for stage in range(stages):
            exchange(g, stage).wait_send()

    @pl.loop(0, fields * nx)
    def _(i):
        store(i).wait()


def solution(mesh):
    slabs, peers = mesh.shape["slab"], mesh.shape["field"]

    def per_device(fields, velocity, diffusivity, noise, mix_rate, evaporation, rate_matrix, stoich, prefactor):
        count, species, nx, nz, ny = fields.shape
        substeps = noise.shape[1]
        reactions = rate_matrix.shape[0]
        groups = species // GROUP
        bits = peers.bit_length() - 1
        vmem = pl.BlockSpec(memory_space=pltpu.VMEM)
        f32, bf16 = jnp.float32, jnp.bfloat16
        dma = pltpu.SemaphoreType.DMA
        return pl.pallas_call(
            functools.partial(kernel, slabs, peers, substeps),
            out_shape=jax.ShapeDtypeStruct(fields.shape, f32),
            in_specs=[
                pl.BlockSpec(memory_space=pl.ANY), vmem, vmem,
                pl.BlockSpec(memory_space=pltpu.SMEM), vmem, vmem, vmem, vmem, vmem,
            ],
            out_specs=pl.BlockSpec(memory_space=pl.ANY),
            scratch_shapes=[
                pltpu.VMEM((substeps + 1, count, species, nx, nz, ny), f32),
                pltpu.VMEM((substeps, 2, count, species, nz, ny), f32),
                pltpu.VMEM((nx, 6, nz, ny), f32),
                pltpu.VMEM((species, nx, nz, ny), f32),
                pltpu.VMEM((bits, species, nx // 2, nz, ny), f32),
                pltpu.VMEM((bits, species, nx // 2, nz, ny), f32),
                pltpu.VMEM((species, nx, nz, ny), f32),
                pltpu.VMEM((count * nx, 2 * species * ROWS, (nz // ROWS) * ny), bf16),
                pltpu.VMEM((count, species, nx, nz, ny), f32),
                pltpu.VMEM((reactions * ROWS, 2 * species * ROWS), bf16),
                pltpu.VMEM((reactions * ROWS, species * ROWS), bf16),
                pltpu.VMEM((species * ROWS, 3 * reactions * ROWS), bf16),
                dma((groups,)),
                dma((count * nx,)),
                dma((substeps, 2, groups)),
                dma((substeps, 2, groups)),
                dma((bits + 1, groups)),
                dma((bits + 1, groups)),
            ],
            compiler_params=pltpu.CompilerParams(
                collective_id=0, has_side_effects=True, vmem_limit_bytes=60 * 1024 * 1024
            ),
        )(
            fields, velocity, diffusivity, noise, mix_rate, evaporation,
            rate_matrix, stoich, prefactor.reshape(1, -1),
        )

    in_specs = (
        P("field", None, "slab", None, None),
        P(None, "slab", None, None),
        P("slab", None, None),
        P("field", None, None),
        P("slab", None, None),
        P("slab", None, None),
        P(),
        P(),
        P(),
    )
    out_specs = P("field", None, "slab", None, None)
    return jax.shard_map(
        per_device, mesh=mesh, in_specs=in_specs, out_specs=out_specs, check_vma=False
    )
```

```python
import functools

import jax
import jax.numpy as jnp
from jax import lax
from jax.experimental import pallas as pl
from jax.experimental.pallas import tpu as pltpu
from jax.sharding import PartitionSpec as P

GROUP = 2
LANES = 8
DELAYS = (2, 2, 2, 2, 2, 2, 2)
ROWS = 8


def schedule(groups, substeps, stages):
    width = min(LANES, groups)
    events = []
    slot = 0
    for first in range(0, groups, width):
        wave = range(first, min(first + width, groups))
        for k in range(substeps):
            for g in wave:
                events.append((slot, 1, "move", g, k))
                if k == substeps - 1:
                    when = slot
                    for stage in range(stages):
                        when += DELAYS[stage % len(DELAYS)]
                        events.append((when, 0, "sum", g, stage))
                slot += 1
    return width, [e[2:] for e in sorted(events, key=lambda e: (e[0], e[1]))]


def expand(small, turned=False):
    rows, cols = small.shape[::-1] if turned else small.shape
    tall = lax.broadcasted_iota(jnp.int32, (rows * ROWS, rows), 0) // ROWS
    pick_row = (tall == lax.broadcasted_iota(jnp.int32, (rows * ROWS, rows), 1)).astype(jnp.bfloat16)
    wide = lax.broadcasted_iota(jnp.int32, (cols, cols * ROWS), 1) // ROWS
    pick_col = (wide == lax.broadcasted_iota(jnp.int32, (cols, cols * ROWS), 0)).astype(jnp.bfloat16)
    half = lax.dot_general(
        pick_row, small, (((1,), (1 if turned else 0,)), ((), ())),
        preferred_element_type=jnp.float32,
    ).astype(jnp.bfloat16)
    full = jnp.dot(half, pick_col, preferred_element_type=jnp.float32)
    shape = (rows * ROWS, cols * ROWS)
    same = (lax.broadcasted_iota(jnp.int32, shape, 0) % ROWS) == (
        lax.broadcasted_iota(jnp.int32, shape, 1) % ROWS
    )
    return jnp.where(same, full, 0.0).astype(jnp.bfloat16)


def halves(value):
    high = value.astype(jnp.bfloat16)
    low = (value - high.astype(jnp.float32)).astype(jnp.bfloat16)
    return high, low


def kernel(
    slabs, peers, substeps,
    x_hbm, vel, diff, noise, rate, vapour, matrix, stoich, pref,
    out_hbm,
    st, halo, planes, part, got, acc, tot, xs, outv, a_one, a_two, b_all,
    in_sem, out_sem, hs_sem, hr_sem, rs_sem, rr_sem,
):
    fields, species, nx, nz, ny = x_hbm.shape
    groups = species // GROUP
    bits = peers.bit_length() - 1
    stages = bits + 1
    half = nx // 2
    total_fields = fields * peers
    blocks = nz // ROWS

    def members(g):
        return pl.ds(g * GROUP, GROUP)

    loads = [
        pltpu.make_async_copy(x_hbm.at[:, members(g)], st.at[0, :, members(g)], in_sem.at[g])
        for g in range(groups)
    ]
    for load in loads:
        load.start()

    me = lax.axis_index("slab")
    seat = lax.axis_index("field")

    def partner(bit):
        step = 1 << bit
        return seat + step * (1 - 2 * ((seat // step) % 2))

    core = seat % 2
    mine = pl.ds(core * half, half)
    theirs = pl.ds((1 - core) * half, half)

    barrier = pltpu.get_barrier_semaphore()

    @pl.when(me > 0)
    def _():
        pl.semaphore_signal(barrier, inc=1, device_id={"slab": me - 1})

    @pl.when(me < slabs - 1)
    def _():
        pl.semaphore_signal(barrier, inc=1, device_id={"slab": me + 1})

    for bit in range(bits):
        pl.semaphore_signal(barrier, inc=1, device_id={"field": partner(bit)})
    has_left = (me + slabs - 1) // slabs
    has_right = 1 - (me + 1) // slabs
    pl.semaphore_wait(barrier, bits + has_left + has_right)

    def to_left(g, k):
        source = x_hbm.at[:, members(g), 0] if k == 0 else st.at[k, :, members(g), 0]
        return pltpu.make_async_remote_copy(
            src_ref=source, dst_ref=halo.at[k, 1, :, members(g)],
            send_sem=hs_sem.at[k, 0, g], recv_sem=hr_sem.at[k, 1, g],
            device_id={"slab": me - 1},
        )

    def to_right(g, k):
        source = x_hbm.at[:, members(g), nx - 1] if k == 0 else st.at[k, :, members(g), nx - 1]
        return pltpu.make_async_remote_copy(
            src_ref=source, dst_ref=halo.at[k, 0, :, members(g)],
            send_sem=hs_sem.at[k, 1, g], recv_sem=hr_sem.at[k, 0, g],
            device_id={"slab": me + 1},
        )

    def send_halo(g, k):
        @pl.when(me > 0)
        def _():
            to_left(g, k).start()

        @pl.when(me < slabs - 1)
        def _():
            to_right(g, k).start()

    def wait_halo(g, k):
        @pl.when(me > 0)
        def _():
            to_right(g, k).wait_recv()

        @pl.when(me < slabs - 1)
        def _():
            to_left(g, k).wait_recv()

    width, events = schedule(groups, substeps, stages)
    for g in range(width):
        send_halo(g, 0)

    @pl.when(me == 0)
    def _():
        for k in range(substeps):
            @pl.loop(0, fields)
            def _(f):
                halo[k, 0, f] = jnp.zeros((species, nz, ny), jnp.float32)

    @pl.when(me == slabs - 1)
    def _():
        for k in range(substeps):
            @pl.loop(0, fields)
            def _(f):
                halo[k, 1, f] = jnp.zeros((species, nz, ny), jnp.float32)

    for x in range(nx):
        d = diff[x]
        for i in range(3):
            planes[x, i] = d - 0.5 * vel[i, x]
        planes[x, 3] = 0.5 * jnp.sqrt(2.0 * d)
        planes[x, 4] = 2.0 * d
        planes[x, 5] = 1.0 - 6.0 * d

    w_high, w_low = halves(matrix[...])
    a_high = expand(w_high, True)
    a_one[...] = jnp.concatenate([a_high, a_high], axis=1)
    a_two[...] = expand(w_low, True)
    s_high, s_low = halves(stoich[...] * pref[...])
    b_high = expand(s_high)
    b_all[...] = jnp.concatenate([b_high, b_high, expand(s_low)], axis=1)

    def exchange(g, stage):
        if stage == 0:
            source, target, bit = part.at[members(g), theirs], got.at[0, members(g)], 0
        elif stage < bits:
            source, target, bit = acc.at[stage - 1, members(g)], got.at[stage, members(g)], stage
        else:
            source, target, bit = tot.at[members(g), mine], tot.at[members(g), mine], 0
        return pltpu.make_async_remote_copy(
            src_ref=source, dst_ref=target,
            send_sem=rs_sem.at[stage, g], recv_sem=rr_sem.at[stage, g],
            device_id={"field": partner(bit)},
        )

    def move(g, k):
        if k == 0:
            loads[g].wait()
        wait_halo(g, k)

        @pl.loop(0, fields)
        def _(f):
            shift = [noise[i, f, k] for i in range(3)]
            for x in range(nx):
                root = planes[x, 3]
                twice = planes[x, 4]
                diag = planes[x, 5]
                ahead = [planes[x, i] + root * shift[i] for i in range(3)]
                behind = [twice - a for a in ahead]
                for s in range(g * GROUP, (g + 1) * GROUP):
                    c = st[k, f, s, x]
                    xa = st[k, f, s, x + 1] if x + 1 < nx else halo[k, 1, f, s]
                    xb = st[k, f, s, x - 1] if x > 0 else halo[k, 0, f, s]
                    ya = pltpu.roll(c, ny - 1, 1)
                    yb = pltpu.roll(c, 1, 1)
                    za = pltpu.roll(c, nz - 1, 0)
                    zb = pltpu.roll(c, 1, 0)
                    st[k + 1, f, s, x] = (
                        (diag * c + (ahead[0] * xa + behind[0] * xb))
                        + (ahead[1] * ya + behind[1] * yb)
                        + (ahead[2] * za + behind[2] * zb)
                    )

        if k < substeps - 1:
            send_halo(g, k + 1)
            if k == substeps - 2 and g + width < groups:
                send_halo(g + width, 0)
        else:
            for s in range(g * GROUP, (g + 1) * GROUP):
                for x in range(nx):
                    part[s, x] = functools.reduce(
                        lambda a, b: a + b, [st[substeps, f, s, x] for f in range(fields)]
                    )
            exchange(g, 0).start()

    def mix(g):
        @pl.loop(0, fields)
        def _(f):
            for x in range(nx):
                half_rate = 0.5 * rate[x]
                for s in range(g * GROUP, (g + 1) * GROUP, 2):
                    pair = []
                    for one in (s, s + 1):
                        m = st[substeps, f, one, x]
                        m = m - half_rate * (m - tot[one, x] * (1.0 / total_fields))
                        if one == 0:
                            m = m + vapour[x]
                        outv[f, one, x] = m
                        pair.append(m)
                    for b in range(blocks):
                        rows = jnp.concatenate([m[b * ROWS:(b + 1) * ROWS] for m in pair], axis=0)
                        high, low = halves(rows)
                        lanes = slice(b * ny, (b + 1) * ny)
                        xs[f * nx + x, s * ROWS:(s + 2) * ROWS, lanes] = high
                        xs[f * nx + x, (species + s) * ROWS:(species + s + 2) * ROWS, lanes] = low

    def reduce_step(g, stage):
        exchange(g, stage).wait_recv()
        if stage == bits:
            mix(g)
            return
        for s in range(g * GROUP, (g + 1) * GROUP):
            held = part[s, mine] if stage == 0 else acc[stage - 1, s]
            value = held + got[stage, s]
            if stage == bits - 1:
                tot[s, mine] = value
            else:
                acc[stage, s] = value
        exchange(g, stage + 1).start()

    for kind, g, k in events:
        if kind == "move":
            move(g, k)
        else:
            reduce_step(g, k)

    def store(i):
        f, x = i // nx, i % nx
        return pltpu.make_async_copy(outv.at[f, :, x], out_hbm.at[f, :, x], out_sem.at[i])

    @pl.loop(0, fields * nx)
    def _(i):
        f, x = i // nx, i % nx
        drive = jnp.dot(a_one[...], xs[i], preferred_element_type=jnp.float32)
        drive = drive + jnp.dot(
            a_two[...], xs[i, : species * ROWS], preferred_element_type=jnp.float32
        )
        speed = jnp.exp(2.0 * jnp.tanh(drive))
        high, low = halves(speed)
        gain = jnp.dot(
            b_all[...], jnp.concatenate([high, low, high], axis=0),
            preferred_element_type=jnp.float32,
        )
        for b in range(blocks):
            piece = gain[:, b * ny:(b + 1) * ny].reshape(species, ROWS, ny)
            outv[f, :, x, b * ROWS:(b + 1) * ROWS] += piece
        store(i).start()

    for k in range(substeps):
        for g in range(groups):
            @pl.when(me > 0)
            def _():
                to_left(g, k).wait_send()

            @pl.when(me < slabs - 1)
            def _():
                to_right(g, k).wait_send()

    for g in range(groups):
        for stage in range(stages):
            exchange(g, stage).wait_send()

    @pl.loop(0, fields * nx)
    def _(i):
        store(i).wait()


def solution(mesh):
    slabs, peers = mesh.shape["slab"], mesh.shape["field"]

    def per_device(fields, velocity, diffusivity, noise, mix_rate, evaporation, rate_matrix, stoich, prefactor):
        count, species, nx, nz, ny = fields.shape
        substeps = noise.shape[1]
        reactions = rate_matrix.shape[0]
        groups = species // GROUP
        bits = peers.bit_length() - 1
        vmem = pl.BlockSpec(memory_space=pltpu.VMEM)
        f32, bf16 = jnp.float32, jnp.bfloat16
        dma = pltpu.SemaphoreType.DMA
        return pl.pallas_call(
            functools.partial(kernel, slabs, peers, substeps),
            out_shape=jax.ShapeDtypeStruct(fields.shape, f32),
            in_specs=[
                pl.BlockSpec(memory_space=pl.ANY), vmem, vmem,
                pl.BlockSpec(memory_space=pltpu.SMEM), vmem, vmem, vmem, vmem, vmem,
            ],
            out_specs=pl.BlockSpec(memory_space=pl.ANY),
            scratch_shapes=[
                pltpu.VMEM((substeps + 1, count, species, nx, nz, ny), f32),
                pltpu.VMEM((substeps, 2, count, species, nz, ny), f32),
                pltpu.VMEM((nx, 6, nz, ny), f32),
                pltpu.VMEM((species, nx, nz, ny), f32),
                pltpu.VMEM((bits, species, nx // 2, nz, ny), f32),
                pltpu.VMEM((bits, species, nx // 2, nz, ny), f32),
                pltpu.VMEM((species, nx, nz, ny), f32),
                pltpu.VMEM((count * nx, 2 * species * ROWS, (nz // ROWS) * ny), bf16),
                pltpu.VMEM((count, species, nx, nz, ny), f32),
                pltpu.VMEM((reactions * ROWS, 2 * species * ROWS), bf16),
                pltpu.VMEM((reactions * ROWS, species * ROWS), bf16),
                pltpu.VMEM((species * ROWS, 3 * reactions * ROWS), bf16),
                dma((groups,)),
                dma((count * nx,)),
                dma((substeps, 2, groups)),
                dma((substeps, 2, groups)),
                dma((bits + 1, groups)),
                dma((bits + 1, groups)),
            ],
            compiler_params=pltpu.CompilerParams(
                collective_id=0, has_side_effects=True, vmem_limit_bytes=60 * 1024 * 1024
            ),
        )(
            fields, velocity, diffusivity, noise.transpose(2, 0, 1), mix_rate, evaporation,
            rate_matrix.T, stoich, prefactor.reshape(1, -1),
        )

    in_specs = (
        P("field", None, "slab", None, None),
        P(None, "slab", None, None),
        P("slab", None, None),
        P("field", None, None),
        P("slab", None, None),
        P("slab", None, None),
        P(),
        P(),
        P(),
    )
    out_specs = P("field", None, "slab", None, None)
    return jax.shard_map(
        per_device, mesh=mesh, in_specs=in_specs, out_specs=out_specs, check_vma=False
    )
```
